768 devices in a mesh: seq: 96 (over y_hi, z, core), tp: 8 (over y_lo, x).
Axes of the slice: x: 4, y: 8 (y_hi: 4, y_lo: 2; y = y_hi * 2 + y_lo), z: 12, core: 2. Of those that a mesh axis runs over, the one named last changes fastest.
Arguments:
- queries: bfloat16 [98304, 4096], P(('seq', 'tp')), may hold values from -170 to 170, as said below
- keys: bfloat16 [98304, 512], P(('seq', 'tp')), may hold values from -6 to 6
- values: bfloat16 [98304, 512], P(('seq', 'tp')), may hold values from -6 to 6
- segments: int32 [98304], replicated, may hold values from 0 to 767, never falling along the last dimension, each value on 1 to 256 neighbouring positions
- out_weight: bfloat16 [4096, 4096], P('tp'), may hold values from -0.75 to 0.75
Outputs:
- mixed: bfloat16 [98304, 4096], P(('seq', 'tp'))
The draws below stay inside these ranges and needn't reach their ends.
Inputs may be any that keep to these rules, and one draw needn't show every extreme that they name: `segments`: document ids never fall along the positions; one document holds at most 256 positions. `queries`: independent entries.
All inputs are finite; a program needn't handle non-finite values.
Results may differ from the reference program's by a relative error of at most 0.014.
Values may be sent and summed in bfloat16 or wider, within the bound.
No kernel may reach another device: no remote copies, remote signals or barrier semaphores. Data moves between devices by JAX's collectives and lax.ppermute only.
A program may use at most 64 MiB of HBM per device.

```python
import math
import jax
import jax.numpy as jnp
import numpy as np
from jax import lax

D = 4096
HQ = 32
KVH = 4
HD = 128
DOC = 256
TOKENS = 98304
N_TP = 8


def draw_queries(key, part):
    shape = (TOKENS, HQ * HD)
    base = jax.random.normal(jax.random.fold_in(key, 13), shape, jnp.float32)
    base = jnp.clip(base, -4.0, 4.0)
    return base.astype(jnp.bfloat16)


def block_scale(rng, extent, split, least, high):
    level = 1.0
    for axis_at, shards_of in split:
        steps = jax.random.uniform(jax.random.fold_in(jax.random.fold_in(rng, 6), axis_at), (shards_of,), jnp.float32, least / len(split), high / len(split))
        level = level * jnp.repeat(jnp.exp(steps), extent[axis_at] // shards_of).reshape((-1,) + (1,) * (len(extent) - 1 - axis_at))
    return level


def length_profile(number_of, total, limit, skew):
    weights = [(1 << 20) // math.isqrt(grade ** skew) + 1 for grade in range(2, number_of + 1)]
    surplus, given = total - limit - (number_of - 1), [1] * (number_of - 1)
    while surplus > 0:
        candidates = [i for i in range(number_of - 1) if given[i] < limit]
        mass, left = sum([weights[i] for i in candidates]), surplus
        for i in candidates:
            addition = min(limit - given[i], max(1, left * weights[i] // mass), surplus)
            given[i] = given[i] + addition
            surplus = surplus - addition
    return np.array([limit] + given)


def ragged(own_key, number_of, total, bound, lean):
    if number_of == 2:
        one = jax.random.randint(own_key, (), max(1, total - bound), min(bound, total - 1) + 1)
        return jnp.stack([one, total - one])
    lengths = jnp.asarray(length_profile(number_of, total, bound, lean), jnp.int32)
    couples = (number_of - 1) // 2
    source_of, receiver = lengths[1:1 + 2 * couples:2], lengths[2:2 + 2 * couples:2]
    room = jnp.minimum(source_of - 1, bound - receiver)
    shifted = jax.random.randint(jax.random.fold_in(own_key, 1), (couples,), 0, 1 << 20) % (room + 1)
    lengths = lengths.at[1:1 + 2 * couples:2].set(source_of - shifted).at[2:2 + 2 * couples:2].set(receiver + shifted)
    return lengths[jax.random.permutation(jax.random.fold_in(own_key, 2), number_of)]


def bell_draw(stream_key, dims, spread, limit, cuts=(), kind=jnp.bfloat16):
    loudness = block_scale(stream_key, dims, cuts, -0.22, 0.18) if cuts else 1.0
    drawn = jax.random.normal(stream_key, dims, jnp.float32) * spread * loudness
    return jnp.minimum(jnp.maximum(drawn, -limit), limit).astype(kind)


def setup_inputs(seed: int = 0) -> dict:
    key_of = jax.random.split(jax.random.key(seed), 6)
    queries = draw_queries(jax.random.fold_in(key_of[5], 71), 0)
    keys = bell_draw(key_of[1], (TOKENS, KVH * HD), 1.0, 6.0, ((0, 768),))
    values = bell_draw(key_of[2], (TOKENS, KVH * HD), 1.0, 6.0, ((0, 768),))
    segments = jnp.searchsorted(jnp.cumsum(ragged(key_of[3], TOKENS * 2 // DOC, TOKENS, DOC, 2)), jnp.arange(TOKENS), side="right").astype(jnp.int32)
    out_weight = bell_draw(key_of[4], (HQ * HD, D), (HD // 2) ** -0.5, 0.75, ((0, 8),))
    return {"queries": queries, "keys": keys, "values": values, "segments": segments, "out_weight": out_weight}


def reference(queries, keys, values, segments, out_weight):
    total = queries.shape[0]
    group_size = HQ // KVH
    tile_rows = DOC // 2
    width = DOC + tile_rows
    inverse_root = HD ** -0.5
    padded_keys = jnp.concatenate([jnp.zeros((DOC, KVH * HD), jnp.bfloat16), keys], 0)
    padded_values = jnp.concatenate([jnp.zeros((DOC, KVH * HD), jnp.bfloat16), values], 0)
    padded_seg = jnp.concatenate([jnp.full((DOC,), -1, jnp.int32), segments.astype(jnp.int32)], 0)

    def attend(index):
        start = (index * tile_rows).astype(jnp.int32)
        query_rows = lax.dynamic_slice_in_dim(queries, start, tile_rows, 0).astype(jnp.float32).reshape(tile_rows, KVH, group_size, HD)
        key_rows = lax.dynamic_slice_in_dim(padded_keys, start, width, 0).astype(jnp.float32).reshape(width, KVH, HD)
        value_rows = lax.dynamic_slice_in_dim(padded_values, start, width, 0).astype(jnp.float32).reshape(width, KVH, HD)
        key_seg = lax.dynamic_slice_in_dim(padded_seg, start, width, 0)
        query_seg = lax.dynamic_slice_in_dim(padded_seg, (start + DOC).astype(jnp.int32), tile_rows, 0)
        query_pos = start + jnp.arange(tile_rows, dtype=jnp.int32)
        key_pos = start - DOC + jnp.arange(width, dtype=jnp.int32)
        allowed = (key_pos[None, :] <= query_pos[:, None]) & (key_seg[None, :] == query_seg[:, None])
        scores = jnp.einsum("tkgd,skd->kgts", query_rows, key_rows) * inverse_root
        scores = jnp.where(allowed[None, None], scores, -1e30)
        top_score = jnp.max(scores, axis=-1, keepdims=True)
        weights = jnp.where(allowed[None, None], jnp.exp(scores - top_score), 0.0)
        denominator = jnp.sum(weights, axis=-1)
        rounded = lax.optimization_barrier(weights.astype(jnp.bfloat16)).astype(jnp.float32)
        output = jnp.einsum("kgts,skd->kgtd", rounded, value_rows) / denominator[..., None]
        output = jnp.transpose(output.astype(jnp.bfloat16), (2, 0, 1, 3))
        return output.reshape(tile_rows, HQ * HD)

    pieces = lax.map(attend, jnp.arange(total // tile_rows, dtype=jnp.int32))
    attended = pieces.reshape(total, HQ * HD)
    columns = HQ * HD // N_TP
    mixed = jnp.zeros((total, out_weight.shape[1]), jnp.float32)
    for owner in range(N_TP):
        partial_value = jnp.dot(attended[:, owner * columns:(owner + 1) * columns], out_weight[owner * columns:(owner + 1) * columns], preferred_element_type=jnp.float32)
        mixed = mixed + lax.optimization_barrier(partial_value.astype(jnp.bfloat16)).astype(jnp.float32)
    return mixed.astype(jnp.bfloat16)
```

```python
import jax
import jax.numpy as jnp
from jax import lax
from jax.experimental import pallas as pl
from jax.experimental.pallas import tpu as pltpu
from jax.sharding import PartitionSpec as P


HD = 128
XN = 4
YN = 8
ZN = 12
CN = 2
B = 128
KV = 4 * HD
NEG = -1e30
LOG2E = 1.4426950408889634


def device_of(x, y, z, c):
    x, y, z = x % XN, y % YN, z % ZN
    return ((y // 2) * ZN * CN + z * CN + c) * 8 + (y % 2) * XN + x


def pairs_of(move):
    found = []
    for x in range(XN):
        for y in range(YN):
            for z in range(ZN):
                for c in range(CN):
                    found.append((device_of(x, y, z, c), device_of(*move(x, y, z, c))))
    return sorted(found)


def along_x(steps):
    return pairs_of(lambda x, y, z, c: (x + (steps if c == 0 else -steps), y, z, c))


def across_y():
    return pairs_of(lambda x, y, z, c: (x, y - 1 if c == 0 else y + 1, z, c))


def ends_to(steps):
    found = []
    for source, target in along_x(steps):
        if source % XN >= 2:
            found.append((source, target))
    return found


def across_cores():
    return pairs_of(lambda x, y, z, c: (x, y, z, 1 - c))


def next_row():
    rows = YN * ZN * CN
    return [(r * XN + x, (r + 1) * XN + x) for r in range(rows - 1) for x in (2, 3)]


def send(value, pairs):
    return lax.ppermute(value, ("seq", "tp"), pairs)


def vmem():
    return pl.BlockSpec(memory_space=pltpu.VMEM)


def smem():
    return pl.BlockSpec(memory_space=pltpu.SMEM)


def shape(rows, cols):
    return jax.ShapeDtypeStruct((rows, cols), jnp.bfloat16)


def kernel(body, out_shape, in_specs, flops=0, limit=8, **rest):
    many = isinstance(out_shape, list)
    return pl.pallas_call(
        body,
        out_shape=out_shape,
        in_specs=in_specs,
        out_specs=[vmem()] * len(out_shape) if many else vmem(),
        cost_estimate=pl.CostEstimate(
            flops=flops, bytes_accessed=1 << 20, transcendentals=0
        ),
        compiler_params=pltpu.CompilerParams(vmem_limit_bytes=limit << 20),
        **rest,
    )


def place(where, step):
    return (where[0] + XN + where[3] * step) % XN


def pack_body(where, q, k, v, raw, *outs):
    y, c = where[1], where[2]
    raw[:, 0:512] = k[...]
    raw[:, 512:1024] = v[...]
    for step in range(XN):
        d = place(where, step)
        out = outs[step]
        own = pl.multiple_of((2 * y + d // 2) * HD, HD)
        oth = pl.multiple_of((2 * (1 - y) + d // 2) * HD, HD)
        for at, (src, col) in enumerate(((k, own), (k, oth), (v, own), (v, oth))):
            out[:, at * HD : (at + 1) * HD] = src[:, pl.ds(col, HD)]
        a = pl.multiple_of((16 * y + 4 * d) * HD, 512)
        b = pl.multiple_of((16 * (1 - y) + 4 * d + 2 * c) * HD, 256)
        e = pl.multiple_of((16 * (1 - y) + 4 * d + 2 * (1 - c)) * HD, 256)
        out[:, KV : KV + 512] = q[:, pl.ds(a, 512)]
        out[:, KV + 512 : KV + 768] = q[:, pl.ds(b, 256)]
        out[:, KV + 768 : KV + 1024] = q[:, pl.ds(e, 256)]


def pack(where, queries, keys, values):
    return kernel(
        pack_body, [shape(B, 1024)] + [shape(B, KV + 1024)] * XN, [smem()] + [vmem()] * 3
    )(where, queries, keys, values)


def cut(where, weight):
    def body(where, weight, left, right, sems):
        row = pl.multiple_of(where[2] * 256, 256)
        copies = [
            pltpu.make_async_copy(
                weight.at[pl.ds(row, 256), pl.ds(first, cols)], out, sems.at[i]
            )
            for i, (first, cols, out) in enumerate(((0, LEFT, left), (LEFT, RIGHT, right)))
        ]
        for copy in copies:
            copy.start()
        for copy in copies:
            copy.wait()

    return kernel(
        body,
        [shape(256, LEFT), shape(256, RIGHT)],
        [smem(), pl.BlockSpec(memory_space=pltpu.HBM)],
        scratch_shapes=[pltpu.SemaphoreType.DMA((2,))],
    )(where, weight)


def pack_before(where, raw):
    def body(where, raw, *outs):
        for step in range(XN):
            d = place(where, step)
            own = 2 * where[1] + d // 2
            oth = 2 * (1 - where[1]) + d // 2
            for at, head in enumerate((own, oth, 4 + own, 4 + oth)):
                col = pl.multiple_of(head * HD, HD)
                outs[step][:, at * HD : (at + 1) * HD] = raw[:, pl.ds(col, HD)]

    return kernel(body, [shape(B, KV)] * XN, [smem(), vmem()])(where, raw)


def attend(where, seg, befores, packs, steps, weight=None):
    count = len(steps)
    load = weight is not None

    def body(where, seg, *refs):
        befores, packs, refs = refs[:XN], refs[XN : 2 * XN], refs[2 * XN :]
        if load:
            source, out, held, buf, sem = refs
            copy = pltpu.make_async_copy(source, held, sem)
            copy.start()
        else:
            out, buf = refs
        for step, ref in enumerate(befores):
            j = place(where, step)

            @pl.when(j >= 2)
            def _():
                buf[j - 2] = ref[...]

        for step, ref in enumerate(packs):
            buf[place(where, step) + 2] = ref[:, 0:KV]
        row = lax.broadcasted_iota(jnp.int32, (B, 3 * B), 0)
        col = lax.broadcasted_iota(jnp.int32, (B, 3 * B), 1)
        causal = (col - 2 * B) <= row
        for i, step in enumerate(steps):
            j = place(where, step)
            seen = []
            for w in range(3):
                at = where[4] + j + w - 2
                ids = jnp.where(at < 0, -1, seg[pl.ds(jnp.maximum(at, 0), 1), :])
                seen.append(jnp.broadcast_to(ids.astype(jnp.float32), (B, B)))
            own_seg = seen[2].T
            same = jnp.concatenate([own_seg - s for s in seen], axis=1) == 0.0
            bias = jnp.where(causal & same, 0.0, NEG)
            bias = jnp.concatenate([bias] * 4, axis=0)
            rows = slice(i * B, (i + 1) * B)
            for g in range(2):
                first = [KV + (g * 4 + h) * HD for h in range(4)]
                qh = jnp.concatenate([packs[step][:, f : f + HD] for f in first], axis=0)
                kh = buf[pl.ds(j, 3), :, g * HD : (g + 1) * HD].reshape(3 * B, HD)
                vh = buf[pl.ds(j, 3), :, (2 + g) * HD : (3 + g) * HD].reshape(3 * B, HD)
                s = lax.dot_general(
                    qh, kh, (((1,), (1,)), ((), ())), preferred_element_type=jnp.float32
                )
                s = s * (LOG2E * HD**-0.5) + bias
                top = jnp.max(s, axis=1, keepdims=True)
                w = jnp.exp2(s - top)
                den = jnp.sum(w, axis=1, keepdims=True)
                o = jnp.dot(w.astype(jnp.bfloat16), vh, preferred_element_type=jnp.float32)
                o = (o / den).astype(jnp.bfloat16)
                for h in range(4):
                    out[rows, (g * 4 + h) * HD : (g * 4 + h + 1) * HD] = o[h * B : (h + 1) * B]
        if load:
            copy.wait()

    scratch = [pltpu.VMEM((6, B, KV), jnp.bfloat16)]
    out_shape = shape(count * B, 1024)
    in_specs = [smem()] + [vmem()] * (1 + 2 * XN)
    operands = [where, seg, *befores, *packs]
    if load:
        scratch.append(pltpu.SemaphoreType.DMA(()))
        out_shape = [out_shape, shape(*weight.shape)]
        in_specs.append(pl.BlockSpec(memory_space=pltpu.HBM))
        operands.append(weight)
    return kernel(
        body, out_shape, in_specs, flops=count * 800000000, limit=8, scratch_shapes=scratch
    )(*operands)


def project(att, w_own, w_mine, w_other, first, cols):
    tile = 256
    blocks = att.shape[0] // B

    def body(att, own, mine, other, *outs):
        for t in range(cols // tile):
            here = slice(t * tile, (t + 1) * tile)
            src = slice(first + t * tile, first + (t + 1) * tile)
            acc = jnp.dot(att[:, 0:512], own[:, src], preferred_element_type=jnp.float32)
            acc += jnp.dot(att[:, 512:768], mine[:, here], preferred_element_type=jnp.float32)
            acc += jnp.dot(att[:, 768:1024], other[:, here], preferred_element_type=jnp.float32)
            acc = acc.astype(jnp.bfloat16)
            for k in range(blocks):
                outs[k][:, here] = acc[k * B : (k + 1) * B]

    return kernel(
        body, [shape(B, cols)] * blocks, [vmem()] * 4, flops=2 * blocks * B * 1024 * cols, limit=6
    )(att, w_own, w_mine, w_other)


def joined_of(own, arrived):
    def body(a, b, out):
        total = a[...].astype(jnp.float32) + b[...].astype(jnp.float32)
        out[...] = total.astype(jnp.bfloat16)

    return kernel(body, shape(*own.shape), [vmem()] * 2)(own, near(arrived))


def finish(parts_l, parts_r):
    def body(*refs):
        out = refs[4]
        for at, (first, cols) in enumerate(((0, LEFT), (LEFT, RIGHT))):
            a, b = (refs[at * 2 + i][...].astype(jnp.float32) for i in range(2))
            out[:, first : first + cols] = (a + b).astype(jnp.bfloat16)

    return kernel(body, shape(B, LEFT + RIGHT), [vmem()] * 4)(*parts_l, *parts_r)


def apart(value):
    return pltpu.with_memory_space_constraint(value, pltpu.HBM)


def near(value):
    return pltpu.with_memory_space_constraint(value, pltpu.VMEM)


LEFT, RIGHT = 2560, 1536


def layer(queries, keys, values, segments, out_weight):
    seq = lax.axis_index("seq")
    tp = lax.axis_index("tp")
    x, y, c = tp % XN, tp // XN, seq % CN
    where = jnp.stack([x, y, c, 1 - 2 * c, seq * 8 + y * XN]).astype(jnp.int32)
    onward, back, far = along_x(1), along_x(-1), along_x(2)

    w_l, w_r = cut(where, apart(out_weight))
    raw, pack0, pack1, pack2, pack3 = pack(where, near(queries), near(keys), near(values))
    raw = near(send(raw, next_row()))
    packs = [
        near(pack0), near(send(pack3, back)), near(send(pack2, far)), near(send(pack1, onward))
    ]
    mine_l = near(send(w_l, across_y()))
    mine_r = near(send(w_r, across_y()))
    before0, before1, before2, before3 = pack_before(where, raw)
    befores = [
        near(before0),
        near(send(before3, ends_to(-1))),
        near(send(before2, ends_to(2))),
        near(send(before1, ends_to(1))),
    ]

    seg = near(segments.reshape(-1, B))

    other_l = near(send(mine_l, across_cores()))
    other_r = near(send(mine_r, across_cores()))

    att_a, w_own = attend(where, seg, befores, packs, (3,), apart(out_weight))
    w_own = near(w_own)
    (p3l,) = project(att_a, w_own, mine_l, other_l, 0, LEFT)
    l1 = send(p3l, onward)
    att_b = attend(where, seg, befores, packs, (2, 1, 0))
    (p3r,) = project(att_a, w_own, mine_r, other_r, LEFT, RIGHT)
    r1 = send(p3r, onward)
    p2l, p1l, p0l = project(att_b, w_own, mine_l, other_l, 0, LEFT)
    p2r, p1r, p0r = project(att_b, w_own, mine_r, other_r, LEFT, RIGHT)
    l2 = send(joined_of(p2l, l1), onward)
    r2 = send(joined_of(p2r, r1), onward)
    l3 = send(joined_of(p1l, l2), onward)
    r3 = send(joined_of(p1r, r2), onward)
    return finish([p0l, near(l3)], [p0r, near(r3)])


def solution(mesh):
    placed = (
        P(("seq", "tp"), None),
        P(("seq", "tp"), None),
        P(("seq", "tp"), None),
        P(),
        P("tp", None),
    )
    return jax.shard_map(
        layer, mesh=mesh, in_specs=placed, out_specs=P(("seq", "tp"), None), check_vma=False
    )
```

```python
import jax
import jax.numpy as jnp
from jax import lax
from jax.experimental import pallas as pl
from jax.experimental.pallas import tpu as pltpu
from jax.sharding import PartitionSpec as P


HD = 128
PARTS = 8
XN = 4
YN = 8
ZN = 12
CN = 2
B = 128
KV = 4 * HD
NEG = -1e30
LOG2E = 1.4426950408889634


def device_of(x, y, z, c):
    x, y, z = x % XN, y % YN, z % ZN
    return ((y // 2) * ZN * CN + z * CN + c) * 8 + (y % 2) * XN + x


def pairs_of(move):
    found = []
    for x in range(XN):
        for y in range(YN):
            for z in range(ZN):
                for c in range(CN):
                    found.append((device_of(x, y, z, c), device_of(*move(x, y, z, c))))
    return sorted(found)


def along_x(steps):
    return pairs_of(lambda x, y, z, c: (x + (steps if c == 0 else -steps), y, z, c))


def across_y():
    return pairs_of(lambda x, y, z, c: (x, y - 1 if c == 0 else y + 1, z, c))


def neighbours():
    return pairs_of(lambda x, y, z, c: (x ^ 1, y, z, c))


def across_cores():
    return pairs_of(lambda x, y, z, c: (x, y, z, 1 - c))


def next_row(shift):
    rows = YN * ZN * CN
    return [(r * XN + x, (r + 1) * XN + x - shift) for r in range(rows - 1) for x in (2, 3)]


def send(value, pairs):
    return lax.ppermute(value, ("seq", "tp"), pairs)


def vmem():
    return pl.BlockSpec(memory_space=pltpu.VMEM)


def smem():
    return pl.BlockSpec(memory_space=pltpu.SMEM)


def shape(rows, cols):
    return jax.ShapeDtypeStruct((rows, cols), jnp.bfloat16)


def kernel(body, out_shape, in_specs, flops=0, limit=8, **rest):
    many = isinstance(out_shape, list)
    return pl.pallas_call(
        body,
        out_shape=out_shape,
        in_specs=in_specs,
        out_specs=[vmem()] * len(out_shape) if many else vmem(),
        cost_estimate=pl.CostEstimate(
            flops=flops, bytes_accessed=1 << 20, transcendentals=0
        ),
        compiler_params=pltpu.CompilerParams(vmem_limit_bytes=limit << 20),
        **rest,
    )


def place(where, step):
    return (where[0] + XN + where[3] * step) % XN


def load(moves, sems):
    copies = []
    for source, target in moves:
        rows = source.shape[0] // PARTS
        for part in range(PARTS):
            here = pl.ds(part * rows, rows)
            copies.append(
                pltpu.make_async_copy(source.at[here], target.at[here], sems.at[len(copies)])
            )
    for copy in copies:
        copy.start()
    return copies


def pack_body(where, q_hbm, k_hbm, v_hbm, w_hbm, *rest):
    outs, (tail_2, tail_0, w_l, w_r, q, k, v, sems, w_sems) = rest[:XN], rest[XN:]
    y, c = where[1], where[2]
    inputs = load(((q_hbm, q), (k_hbm, k), (v_hbm, v)), sems)
    rows = pl.ds(pl.multiple_of(c * 256, 256), 256)
    weights = load(
        (
            (w_hbm.at[rows, pl.ds(0, LEFT)], w_l),
            (w_hbm.at[rows, pl.ds(LEFT, RIGHT)], w_r),
        ),
        w_sems,
    )
    for copy in inputs:
        copy.wait()

    def heads_of(d, out):
        own = pl.multiple_of((2 * y + d // 2) * HD, HD)
        oth = pl.multiple_of((2 * (1 - y) + d // 2) * HD, HD)
        for at, (src, col) in enumerate(((k, own), (k, oth), (v, own), (v, oth))):
            out[:, at * HD : (at + 1) * HD] = src[:, pl.ds(col, HD)]

    heads_of(2, tail_2)
    heads_of(0, tail_0)
    for step in range(XN):
        d = place(where, step)
        out = outs[step]
        heads_of(d, out)
        a = pl.multiple_of((16 * y + 4 * d) * HD, 512)
        b = pl.multiple_of((16 * (1 - y) + 4 * d + 2 * c) * HD, 256)
        e = pl.multiple_of((16 * (1 - y) + 4 * d + 2 * (1 - c)) * HD, 256)
        out[:, KV : KV + 512] = q[:, pl.ds(a, 512)]
        out[:, KV + 512 : KV + 768] = q[:, pl.ds(b, 256)]
        out[:, KV + 768 : KV + 1024] = q[:, pl.ds(e, 256)]
    for copy in weights:
        copy.wait()


def pack(where, queries, keys, values, weight):
    hbm = pl.BlockSpec(memory_space=pltpu.HBM)
    return kernel(
        pack_body,
        [shape(B, KV + 1024)] * XN
        + [shape(B, KV)] * 2
        + [shape(256, LEFT), shape(256, RIGHT)],
        [smem()] + [hbm] * 4,
        scratch_shapes=[
            pltpu.VMEM((B, 4096), jnp.bfloat16),
            pltpu.VMEM((B, 512), jnp.bfloat16),
            pltpu.VMEM((B, 512), jnp.bfloat16),
            pltpu.SemaphoreType.DMA((3 * PARTS,)),
            pltpu.SemaphoreType.DMA((2 * PARTS,)),
        ],
    )(where, queries, keys, values, weight)


def pick(where, low, high):
    def body(where, low, high, out):
        @pl.when(where[0] < 2)
        def _():
            out[...] = low[...]

        @pl.when(where[0] >= 2)
        def _():
            out[...] = high[...]

    return kernel(body, shape(*low.shape), [smem(), vmem(), vmem()])(where, low, high)


def attend(where, seg, befores, packs, steps):
    count = len(steps)

    def body(where, seg, *refs):
        (mine, other), packs, refs = refs[:2], refs[2 : 2 + XN], refs[2 + XN :]
        out, buf = refs
        odd = where[0] % 2
        for ref, slot in ((mine, odd), (other, 1 - odd)):
            for at in range(4):
                buf[slot, :, at * HD : (at + 1) * HD] = ref[:, (at ^ 1) * HD : ((at ^ 1) + 1) * HD]
        for step, ref in enumerate(packs):
            buf[place(where, step) + 2] = ref[:, 0:KV]
        row = lax.broadcasted_iota(jnp.int32, (B, 3 * B), 0)
        col = lax.broadcasted_iota(jnp.int32, (B, 3 * B), 1)
        causal = (col - 2 * B) <= row
        for i, step in enumerate(steps):
            j = place(where, step)
            seen = []
            for w in range(3):
                at = where[4] + j + w - 2
                ids = jnp.where(at < 0, -1, seg[pl.ds(jnp.maximum(at, 0), 1), :])
                seen.append(jnp.broadcast_to(ids.astype(jnp.float32), (B, B)))
            own_seg = seen[2].T
            same = jnp.concatenate([own_seg - s for s in seen], axis=1) == 0.0
            bias = jnp.where(causal & same, 0.0, NEG)
            bias = jnp.concatenate([bias] * 4, axis=0)
            rows = slice(i * B, (i + 1) * B)
            for g in range(2):
                starts = [KV + (g * 4 + h) * HD for h in range(4)]
                qh = jnp.concatenate([packs[step][:, f : f + HD] for f in starts], axis=0)
                kh = buf[pl.ds(j, 3), :, g * HD : (g + 1) * HD].reshape(3 * B, HD)
                vh = buf[pl.ds(j, 3), :, (2 + g) * HD : (3 + g) * HD].reshape(3 * B, HD)
                s = lax.dot_general(
                    qh, kh, (((1,), (1,)), ((), ())), preferred_element_type=jnp.float32
                )
                s = s * (LOG2E * HD**-0.5) + bias
                top = jnp.max(s, axis=1, keepdims=True)
                w = jnp.exp2(s - top)
                den = jnp.sum(w, axis=1, keepdims=True)
                o = jnp.dot(w.astype(jnp.bfloat16), vh, preferred_element_type=jnp.float32)
                o = (o / den).astype(jnp.bfloat16)
                for h in range(4):
                    out[rows, (g * 4 + h) * HD : (g * 4 + h + 1) * HD] = o[h * B : (h + 1) * B]

    return kernel(
        body,
        shape(count * B, 1024),
        [smem()] + [vmem()] * (3 + XN),
        flops=count * 800000000,
        limit=8,
        scratch_shapes=[pltpu.VMEM((6, B, KV), jnp.bfloat16)],
    )(where, seg, *befores, *packs)


def project(att, w_own, w_mine, w_other, first, cols):
    tile = 256
    blocks = att.shape[0] // B

    def body(att, own, mine, other, *outs):
        for t in range(cols // tile):
            here = slice(t * tile, (t + 1) * tile)
            acc = jnp.dot(att[:, 0:512], own[:, first + t * tile : first + (t + 1) * tile], preferred_element_type=jnp.float32)
            acc += jnp.dot(att[:, 512:768], mine[:, here], preferred_element_type=jnp.float32)
            acc += jnp.dot(att[:, 768:1024], other[:, here], preferred_element_type=jnp.float32)
            acc = acc.astype(jnp.bfloat16)
            for k in range(blocks):
                outs[k][:, here] = acc[k * B : (k + 1) * B]

    return kernel(
        body, [shape(B, cols)] * blocks, [vmem()] * 4, flops=2 * blocks * B * 1024 * cols, limit=6
    )(att, w_own, w_mine, w_other)


def joined_of(own, arrived):
    def body(a, b, out):
        total = a[...].astype(jnp.float32) + b[...].astype(jnp.float32)
        out[...] = total.astype(jnp.bfloat16)

    return kernel(body, shape(*own.shape), [vmem()] * 2)(own, near(arrived))


def finish(part, arrived, first, held=None):
    cols = part.shape[1]

    def body(*refs):
        a, b = refs[:2]
        out, total, sem = refs[-3:]
        total[...] = (a[...].astype(jnp.float32) + b[...].astype(jnp.float32)).astype(
            jnp.bfloat16
        )
        copy = pltpu.make_async_copy(total, out.at[:, pl.ds(first, cols)], sem)
        copy.start()
        copy.wait()

    hbm = pl.BlockSpec(memory_space=pltpu.HBM)
    again = held is not None
    return pl.pallas_call(
        body,
        out_shape=shape(B, LEFT + RIGHT),
        in_specs=[vmem(), vmem()] + [hbm] * again,
        out_specs=hbm,
        input_output_aliases={2: 0} if again else {},
        scratch_shapes=[pltpu.VMEM((B, cols), jnp.bfloat16), pltpu.SemaphoreType.DMA(())],
        compiler_params=pltpu.CompilerParams(vmem_limit_bytes=8 << 20),
        name="finish",
    )(part, arrived, *([held] if again else []))


def apart(value):
    return pltpu.with_memory_space_constraint(value, pltpu.HBM)


def near(value):
    return pltpu.with_memory_space_constraint(value, pltpu.VMEM)


LEFT, RIGHT = 2304, 1792


def layer(queries, keys, values, segments, out_weight):
    seq = lax.axis_index("seq")
    tp = lax.axis_index("tp")
    x, y, c = tp % XN, tp // XN, seq % CN
    where = jnp.stack([x, y, c, 1 - 2 * c, seq * 8 + y * XN]).astype(jnp.int32)
    onward, back, far = along_x(1), along_x(-1), along_x(2)

    weight = apart(out_weight)
    pack0, pack1, pack2, pack3, tail_2, tail_0, w_l, w_r = pack(
        where, apart(queries), apart(keys), apart(values), weight
    )
    tail_2 = near(send(tail_2, next_row(0)))
    tail_0 = near(send(tail_0, next_row(2)))
    packs = [
        near(pack0), near(send(pack3, back)), near(send(pack2, far)), near(send(pack1, onward))
    ]
    mine_l = near(send(w_l, across_y()))
    mine_r = near(send(w_r, across_y()))
    before = near(pick(where, tail_0, tail_2))
    befores = [before, near(send(before, neighbours()))]

    seg = near(segments.reshape(-1, B))

    other_l = near(send(mine_l, across_cores()))
    other_r = near(send(mine_r, across_cores()))

    att_a = attend(where, seg, befores, packs, (3,))
    (p3l,) = project(att_a, out_weight, mine_l, other_l, 0, LEFT)
    l1 = send(p3l, onward)
    att_b = attend(where, seg, befores, packs, (2, 1, 0))
    (p3r,) = project(att_a, out_weight, mine_r, other_r, LEFT, RIGHT)
    r1 = send(p3r, onward)
    p2l, p1l, p0l = project(att_b, out_weight, mine_l, other_l, 0, LEFT)
    p2r, p1r, p0r = project(att_b, out_weight, mine_r, other_r, LEFT, RIGHT)
    l2 = send(joined_of(p2l, l1), onward)
    r2 = send(joined_of(p2r, r1), onward)
    l3 = send(joined_of(p1l, l2), onward)
    r3 = send(joined_of(p1r, r2), onward)
    out = finish(p0l, near(l3), 0)
    return finish(p0r, near(r3), LEFT, out)


def solution(mesh):
    placed = (
        P(("seq", "tp"), None),
        P(("seq", "tp"), None),
        P(("seq", "tp"), None),
        P(),
        P("tp", None),
    )
    return jax.shard_map(
        layer, mesh=mesh, in_specs=placed, out_specs=P(("seq", "tp"), None), check_vma=False
    )
```
